32 devices in a mesh: pole: 2 (over y), leaf: 16 (over z, x, core).
Axes of the slice: x: 2, y: 2, z: 4, core: 2. Of those that a mesh axis runs over, the one named last changes fastest.
Arguments:
- root_frame: float32 [2048, 1024], P(('pole', 'leaf')), parts along dimension 0, may hold values from -2 to 8, as said below
- top_lhat: float32 [3072, 256], P(('pole', 'leaf')), parts along dimension 0, may hold values from -0.21875 to 0.21875
- top_dinv: float32 [1024, 256], P(('pole', 'leaf')), parts along dimension 0, may hold values from -2 to 8, as said below
- mid_lhat: float32 [32, 768, 256], P(('pole', 'leaf')), parts along dimension 0, may hold values from -0.21875 to 0.21875
- mid_dinv: float32 [32, 256, 256], P(('pole', 'leaf')), parts along dimension 0, may hold values from -2 to 8, as said below
- leaf_lhat: float32 [64, 768, 256], P(('pole', 'leaf')), parts along dimension 0, may hold values from -0.21875 to 0.21875
- leaf_dinv: float32 [64, 256, 256], P(('pole', 'leaf')), parts along dimension 0, may hold values from -2 to 8, as said below
- top_columns: int32 [2], replicated, may hold values from 128 to 256
- mid_columns: int32 [16], replicated, may hold values from 128 to 256
- leaf_columns: int32 [32], replicated, may hold values from 128 to 256
- top_pattern: int32 [2, 3], replicated, may hold values from 0 to 3, as said below
- mid_parent: int32 [16], replicated, may hold values from 0 to 1, as said below
- leaf_parent: int32 [32], replicated, may hold values from 0 to 15, as said below
- mid_pattern: int32 [16, 3], replicated, may hold values from 0 to 3, as said below
- leaf_pattern: int32 [32, 3], replicated, may hold values from 0 to 3, as said below
- leaf_live: int32 [16], replicated, may hold values from 1 to 2, as said below
Outputs:
- top_diagonal: float32 [1024, 256], P(('pole', 'leaf')), parts along dimension 0
- top_coupling: float32 [3072, 256], P(('pole', 'leaf')), parts along dimension 0
- mid_diagonal: float32 [32, 256, 256], P(('pole', 'leaf')), parts along dimension 0
- mid_coupling: float32 [32, 768, 256], P(('pole', 'leaf')), parts along dimension 0
- leaf_diagonal: float32 [64, 256, 256], P(('pole', 'leaf')), parts along dimension 0
- leaf_coupling: float32 [64, 768, 256], P(('pole', 'leaf')), parts along dimension 0
The draws below stay inside these ranges and needn't reach their ends.
There are 2 independent parts, one for each index of `pole`. The reference program is written for one: setup_inputs(seed, part) draws one part's arguments, and reference() takes and returns one part's arrays. A program takes and returns all parts, laid end to end along the dimension named above; an argument that names none is the same for every part. Nothing has to cross between parts.
Inputs may be any that keep to these rules, and one draw needn't show every extreme that they name: `root_frame`: Symmetric. `top_dinv`: each 256 x 256 block is symmetric. `mid_dinv`: each block is symmetric. `leaf_dinv`: each block is symmetric. `top_pattern`: each row holds 3 distinct increasing numbers of 0 to 3. mid_parent[j] is 2 * (j // 16) plus a number below 2: a level-1 supernode hangs under a level-2 supernode of its own group of 16 devices. leaf_parent[i] is one of the 4 level-1 supernodes numbered from 4 * (i // 8): a leaf hangs under a level-1 supernode of its own group of 4 devices. `mid_pattern`: each row starts with 0 (the parent) and goes on with 2 distinct increasing numbers of 1 to 3. `leaf_pattern`: each row starts with 0 (the parent) and goes on with 2 distinct increasing numbers of 1 to 3. The leaf supernodes of device d are its first leaf_live[d] slots; some device has all 2.
All inputs are finite; a program needn't handle non-finite values.
Results may differ from the reference program's by a relative error of at most 0.0003.
Values sent between devices are 32-bit elements; how exact they have to be, the bound alone decides.
A program may use at most 128 MiB of HBM per device.

```python
import jax
import jax.numpy as jnp
from jax import lax

COLS = 256
SLOTS = 3
GROUP2 = 16
NODES2 = 2
GROUP1 = 4
L0_DEV = 2
ROOTB = 4
TOP = 2
MID = 16
LEAFS = 32


def symmetric_blocks(key, number, extent):
    noise_key, scale_key = jax.random.split(key)
    noise = jax.random.normal(noise_key, (number, extent, extent), jnp.float32)
    diagonal = jax.random.uniform(scale_key, (number, extent), jnp.float32, 1.0, 3.0)
    twin = (noise + jnp.swapaxes(noise, 1, 2)) * (0.45 / jnp.sqrt(extent * 1.0))
    return twin + diagonal[:, :, None] * jnp.eye(extent, dtype=jnp.float32)[None]


def draw_root_frame(key, part):
    blocks = symmetric_blocks(jax.random.fold_in(key, 11), 1, ROOTB * COLS)
    return blocks.reshape(ROOTB * COLS, ROOTB * COLS)


def draw_top_dinv(key, part):
    blocks = symmetric_blocks(jax.random.fold_in(key, 12), TOP, COLS)
    return blocks.reshape(TOP * COLS, COLS)


def draw_mid_dinv(key, part):
    return symmetric_blocks(jax.random.fold_in(key, 13), MID, COLS)


def draw_leaf_dinv(key, part):
    return symmetric_blocks(jax.random.fold_in(key, 14), LEAFS, COLS)


def draw_top_pattern(key, part):
    skipped = jax.random.randint(jax.random.fold_in(key, 33), (TOP, 1), 0, SLOTS + 1)
    later = jnp.arange(0, SLOTS, dtype=jnp.int32)[None, :]
    return (later + (later >= skipped).astype(jnp.int32)).astype(jnp.int32)


def draw_mid_parent(key, part):
    offsets = jax.random.randint(jax.random.fold_in(key, 21), (MID,), 0, NODES2)
    return (jnp.arange(MID, dtype=jnp.int32) // GROUP2 * NODES2 + offsets).astype(jnp.int32)


def draw_leaf_parent(key, part):
    holder = jnp.arange(LEAFS, dtype=jnp.int32) // L0_DEV
    offsets = jax.random.randint(jax.random.fold_in(key, 22), (LEAFS,), 0, GROUP1)
    return (holder // GROUP1 * GROUP1 + offsets).astype(jnp.int32)


def pattern_rows(key, number):
    skipped = jax.random.randint(key, (number, 1), 1, SLOTS + 1)
    later = jnp.arange(1, SLOTS, dtype=jnp.int32)[None, :]
    remaining = later + (later >= skipped).astype(jnp.int32)
    return jnp.concatenate([jnp.zeros((number, 1), jnp.int32), remaining], axis=1).astype(jnp.int32)


def draw_mid_pattern(key, part):
    return pattern_rows(jax.random.fold_in(key, 31), MID)


def draw_leaf_pattern(key, part):
    return pattern_rows(jax.random.fold_in(key, 32), LEAFS)


def draw_leaf_live(key, part):
    first_key, second_key, peak_key = jax.random.split(jax.random.fold_in(key, 41), 3)
    lower_count = jnp.minimum(jax.random.randint(first_key, (MID,), 0, L0_DEV), jax.random.randint(second_key, (MID,), 0, L0_DEV)) + 1
    peak_device = jax.random.randint(peak_key, (), 0, MID)
    return jnp.where(jnp.arange(MID, dtype=jnp.int32) == peak_device, L0_DEV, lower_count).astype(jnp.int32)


def with_ends(array, rng, least, high):
    dims = array.shape
    place = [jax.random.randint(jax.random.fold_in(rng, axis), (), 0, dims[axis]) for axis in range(len(dims))]
    array = array.at[tuple(place)].set(least)
    longest = dims.index(max(dims))
    place[longest] = (place[longest] + 1) % dims[longest]
    return array.at[tuple(place)].set(high)


def level_of(rng, shape, cuts, low, top_value):
    loudness = 1.0
    for position, shards_of in cuts:
        draws = jax.random.uniform(jax.random.fold_in(jax.random.fold_in(rng, 6), position), (shards_of,), jnp.float32, low / len(cuts), top_value / len(cuts))
        loudness = loudness * jnp.repeat(jnp.exp(draws), shape[position] // shards_of).reshape((-1,) + (1,) * (len(shape) - 1 - position))
    return loudness


def bell_draw(own_key, shape, scale, bound, shards=(), held_as=jnp.bfloat16):
    drawn = scale * jax.random.normal(own_key, shape, jnp.float32)
    if shards:
        drawn = drawn * level_of(own_key, shape, shards, -0.22, 0.18)
    return jnp.clip(drawn, -bound, bound).astype(held_as)


def setup_inputs(seed: int = 0, part: int = 0) -> dict:
    keys = jax.random.split(jax.random.key(seed), 17)
    part_splits = jax.random.split(jax.random.fold_in(keys[16], part), 17)
    root_frame = draw_root_frame(jax.random.fold_in(jax.random.fold_in(keys[16], part), 71), part)
    top_lhat = bell_draw(part_splits[1], (TOP * SLOTS * COLS, COLS), (SLOTS * COLS) ** -0.5, 0.21875, ((0, 16),), jnp.float32)
    top_dinv = draw_top_dinv(jax.random.fold_in(jax.random.fold_in(keys[16], part), 71), part)
    mid_lhat = bell_draw(part_splits[3], (MID, SLOTS * COLS, COLS), (SLOTS * COLS) ** -0.5, 0.21875, ((0, 16),), jnp.float32)
    mid_dinv = draw_mid_dinv(jax.random.fold_in(jax.random.fold_in(keys[16], part), 71), part)
    leaf_lhat = bell_draw(part_splits[5], (LEAFS, SLOTS * COLS, COLS), (SLOTS * COLS) ** -0.5, 0.21875, ((0, 16),), jnp.float32)
    leaf_dinv = draw_leaf_dinv(jax.random.fold_in(jax.random.fold_in(keys[16], part), 71), part)
    top_columns = jax.random.randint(keys[7], (TOP,), COLS // 2, COLS + 1).astype(jnp.int32)
    mid_columns = with_ends(jax.random.randint(keys[8], (MID,), COLS // 2, COLS + 1), jax.random.fold_in(keys[8], 1), COLS // 2, COLS).astype(jnp.int32)
    leaf_columns = with_ends(jax.random.randint(keys[9], (LEAFS,), COLS // 2, COLS + 1), jax.random.fold_in(keys[9], 1), COLS // 2, COLS).astype(jnp.int32)
    top_pattern = draw_top_pattern(jax.random.fold_in(keys[16], 71), part)
    mid_parent = draw_mid_parent(jax.random.fold_in(keys[16], 71), part)
    leaf_parent = draw_leaf_parent(jax.random.fold_in(keys[16], 71), part)
    mid_pattern = draw_mid_pattern(jax.random.fold_in(keys[16], 71), part)
    leaf_pattern = draw_leaf_pattern(jax.random.fold_in(keys[16], 71), part)
    leaf_live = draw_leaf_live(jax.random.fold_in(keys[16], 71), part)
    return dict(root_frame=root_frame, top_lhat=top_lhat, top_dinv=top_dinv, mid_lhat=mid_lhat, mid_dinv=mid_dinv, leaf_lhat=leaf_lhat, leaf_dinv=leaf_dinv, top_columns=top_columns, mid_columns=mid_columns, leaf_columns=leaf_columns, top_pattern=top_pattern, mid_parent=mid_parent, leaf_parent=leaf_parent, mid_pattern=mid_pattern, leaf_pattern=leaf_pattern, leaf_live=leaf_live)


highest = lax.Precision.HIGHEST


def masked_inputs(lhat_block, dinv_block, used_width):
    block_size = lhat_block.shape[-1]
    column_keep = (jnp.arange(block_size, dtype=jnp.int32) < used_width).astype(lhat_block.dtype)
    lhat_masked = lhat_block * column_keep[None, :]
    dinv_masked = dinv_block * column_keep[:, None] * column_keep[None, :]
    return lhat_masked, dinv_masked


def solve_node(local_frame, lhat_block, dinv_block, used_width):
    lhat_masked, dinv_masked = masked_inputs(lhat_block, dinv_block, used_width)
    coupling = -jnp.dot(local_frame, lhat_masked, precision=highest, preferred_element_type=jnp.float32)
    diagonal = dinv_masked - jnp.dot(lhat_masked.T, coupling, precision=highest, preferred_element_type=jnp.float32)
    return diagonal, coupling


def extended_matrix(diagonal, coupling, local_frame):
    upper_row = jnp.concatenate([diagonal, coupling.T], axis=1)
    lower_row = jnp.concatenate([coupling, local_frame], axis=1)
    return jnp.concatenate([upper_row, lower_row], axis=0)


def select_frame(matrix, pattern, block_size):
    row_ids = (pattern[:, None].astype(jnp.int32) * block_size + jnp.arange(block_size, dtype=jnp.int32)[None, :]).reshape(-1).astype(jnp.int32)
    picked = jnp.take(matrix, row_ids, axis=0)
    return jnp.take(picked, row_ids, axis=1)


def reference(root_frame, top_lhat, top_dinv, mid_lhat, mid_dinv, leaf_lhat, leaf_dinv, top_columns, mid_columns, leaf_columns, top_pattern, mid_parent, leaf_parent, mid_pattern, leaf_pattern, leaf_live):
    frame_size = SLOTS * COLS
    frame_nodes = lax.map(lambda pattern: select_frame(root_frame, pattern, COLS), top_pattern)
    lhat_nodes = top_lhat.reshape(TOP, frame_size, COLS)
    dinv_nodes = top_dinv.reshape(TOP, COLS, COLS)
    top_diag, top_coup = jax.vmap(solve_node)(frame_nodes, lhat_nodes, dinv_nodes, top_columns)
    upper_mats = jax.vmap(extended_matrix)(top_diag, top_coup, frame_nodes)

    def mid_one(node_index):
        parent = mid_parent[node_index]
        local_frame = select_frame(upper_mats[parent], mid_pattern[node_index], COLS)
        return solve_node(local_frame, mid_lhat[node_index], mid_dinv[node_index], mid_columns[node_index])

    mid_diag, mid_coup = lax.map(mid_one, jnp.arange(MID, dtype=jnp.int32))

    def leaf_one(node_index):
        parent = leaf_parent[node_index]
        above_frame = select_frame(upper_mats[mid_parent[parent]], mid_pattern[parent], COLS)
        matrix = extended_matrix(mid_diag[parent], mid_coup[parent], above_frame)
        local_frame = select_frame(matrix, leaf_pattern[node_index], COLS)
        diagonal, coupling = solve_node(local_frame, leaf_lhat[node_index], leaf_dinv[node_index], leaf_columns[node_index])
        live_mask = (node_index % L0_DEV < leaf_live[node_index // L0_DEV]).astype(diagonal.dtype)
        return diagonal * live_mask, coupling * live_mask

    leaf_diag, leaf_coup = lax.map(leaf_one, jnp.arange(LEAFS, dtype=jnp.int32))
    return (top_diag.reshape(TOP * COLS, COLS), top_coup.reshape(TOP * frame_size, COLS), mid_diag, mid_coup, leaf_diag, leaf_coup)
```

```python
import functools

import jax
import jax.numpy as jnp
from jax import lax
from jax.experimental import pallas as pl
from jax.experimental.pallas import tpu as pltpu
from jax.sharding import PartitionSpec as P

SLOTS = 3
GROUP2 = 16
NODES2 = 2
GROUP1 = 4

MESH = pl.DeviceIdType.MESH
f32 = jnp.float32
bf16 = jnp.bfloat16


def split(value):
    high = value.astype(bf16)
    low = (value - high.astype(f32)).astype(bf16)
    return high, low


def remote(src, dst, send_sem, recv_sem, target):
    return pltpu.make_async_remote_copy(
        src_ref=src,
        dst_ref=dst,
        send_sem=send_sem,
        recv_sem=recv_sem,
        device_id={"leaf": target},
        device_id_type=MESH,
    )


class Spread:
    def __init__(self, own, whole, group, sems, me):
        self.own, self.whole, self.group = own, whole, group
        self.rows = own.shape[0]
        self.recv, self.up, self.down, self.side, self.core, self.local = sems
        self.base = me - lax.rem(me, group)

    def block(self, device):
        start = (device - self.base) * self.rows
        return self.whole.at[pl.ds(pl.multiple_of(start, 8), self.rows)]

    def copy(self, device, target, sems, own=False):
        slot = device - self.base
        return remote(
            self.own if own else self.block(device),
            self.block(device),
            sems.at[slot],
            self.recv.at[slot],
            target,
        )

    def keep(self, me):
        return pltpu.make_async_copy(self.own, self.block(me), self.local.at[0])

    def arrived(self, device, me):
        self.copy(device, me, self.core).wait_recv()


def gather_kernel(
    n,
    root_in,
    tl_in,
    td_in,
    ml_in,
    md_in,
    root_all,
    tl_all,
    td_all,
    ml_all,
    md_all,
    *sems,
):
    me = lax.axis_index("leaf")
    core = lax.rem(me, 2)
    side = lax.rem(me // 2, 2)
    cpeer = me + 1 - 2 * core
    xpeer = me + 2 - 4 * side
    root = Spread(root_in, root_all, n, sems[0:6], me)
    tl = Spread(tl_in, tl_all, GROUP2, sems[6:12], me)
    td = Spread(td_in, td_all, GROUP2, sems[12:18], me)
    ml = Spread(ml_in, ml_all, GROUP1, sems[18:24], me)
    md = Spread(md_in, md_all, GROUP1, sems[24:30], me)
    tops = (tl, td)
    mids = (ml, md)

    line = n // GROUP1
    place = me // GROUP1
    top_line = GROUP2 // GROUP1
    top_place = lax.rem(me, GROUP2) // GROUP1
    has_up = place < line - 1
    has_down = place > 0

    barrier = pltpu.get_barrier_semaphore()
    for peer in (cpeer, xpeer):
        pl.semaphore_signal(barrier, inc=1, device_id={"leaf": peer}, device_id_type=MESH)

    @pl.when(has_up)
    def _():
        pl.semaphore_signal(barrier, inc=1, device_id={"leaf": me + GROUP1}, device_id_type=MESH)

    @pl.when(has_down)
    def _():
        pl.semaphore_signal(barrier, inc=1, device_id={"leaf": me - GROUP1}, device_id_type=MESH)

    for part in (root,) + tops + mids:
        part.keep(me).start()
    peers = 2 + jnp.minimum(place, 1) + jnp.minimum(line - 1 - place, 1)
    pl.semaphore_wait(barrier, peers)

    def along(part, device, go_up, ok, act, own=False):
        if go_up:
            @pl.when(ok)
            def _():
                act(part.copy(device, me + GROUP1, part.up, own))
        else:
            @pl.when(ok)
            def _():
                act(part.copy(device, me - GROUP1, part.down, own))

    def start(copy):
        copy.start()

    def wait_send(copy):
        copy.wait_send()

    top_up = top_place < top_line - 1
    top_down = top_place > 0

    def own_copies(act):
        act(root.copy(me, xpeer, root.side, True))
        for part in tops:
            along(part, me, True, top_up, act, True)
            along(part, me, False, top_down, act, True)
        along(root, me, True, has_up, act, True)
        along(root, me, False, has_down, act, True)
        for part in tops:
            act(part.copy(me, xpeer, part.side, True))
        for part in (root,) + tops:
            act(part.copy(me, cpeer, part.core, True))
        for part in mids:
            act(part.copy(me, xpeer, part.side, True))
            act(part.copy(me, cpeer, part.core, True))

    own_copies(start)

    root.arrived(xpeer, me)
    along(root, xpeer, True, has_up, start)
    along(root, xpeer, False, has_down, start)
    root.copy(xpeer, cpeer, root.core).start()

    def step(s, carry):
        for go_up in (True, False):
            shift = -s * GROUP1 if go_up else s * GROUP1
            got_top = (top_place >= s) if go_up else (top_place + s < top_line)
            got_root = (place >= s) if go_up else (place + s < line)

            @pl.when(got_top)
            def _():
                for part in tops:
                    part.arrived(me + shift, me)
                    along(part, me + shift, go_up, top_up if go_up else top_down, start)
                    part.copy(me + shift, xpeer, part.side).start()
                    part.copy(me + shift, cpeer, part.core).start()

            @pl.when(got_root)
            def _():
                for device in (me, xpeer):
                    root.arrived(device + shift, me)
                    along(root, device + shift, go_up, has_up if go_up else has_down, start)
                    root.copy(device + shift, cpeer, root.core).start()

        return carry

    lax.fori_loop(1, line, step, 0)

    for part in tops:
        for q in range(top_line):
            device = part.base + q * GROUP1 + lax.rem(xpeer, GROUP1)
            part.arrived(device, me)
            part.copy(device, cpeer, part.core).start()
    for part in (root,) + tops:
        def other(q, carry):
            for peer in (cpeer, cpeer + xpeer - me):
                part.arrived(part.base + q * GROUP1 + lax.rem(peer, GROUP1), me)
            return carry

        lax.fori_loop(0, part.group // GROUP1, other, 0)
        part.keep(me).wait()

    for part in mids:
        part.arrived(xpeer, me)
        part.copy(xpeer, cpeer, part.core).start()
    for part in mids:
        part.arrived(cpeer, me)
        part.arrived(cpeer + xpeer - me, me)
        part.keep(me).wait()

    own_copies(wait_send)
    along(root, xpeer, True, has_up, wait_send)
    along(root, xpeer, False, has_down, wait_send)
    root.copy(xpeer, cpeer, root.core).wait_send()

    def drain(s, carry):
        for go_up in (True, False):
            shift = -s * GROUP1 if go_up else s * GROUP1
            got_top = (top_place >= s) if go_up else (top_place + s < top_line)
            got_root = (place >= s) if go_up else (place + s < line)

            @pl.when(got_top)
            def _():
                for part in tops:
                    along(part, me + shift, go_up, top_up if go_up else top_down, wait_send)
                    part.copy(me + shift, xpeer, part.side).wait_send()
                    part.copy(me + shift, cpeer, part.core).wait_send()

            @pl.when(got_root)
            def _():
                for device in (me, xpeer):
                    along(root, device + shift, go_up, has_up if go_up else has_down, wait_send)
                    root.copy(device + shift, cpeer, root.core).wait_send()

        return carry

    lax.fori_loop(1, line, drain, 0)
    for part in tops:
        for q in range(top_line):
            device = part.base + q * GROUP1 + lax.rem(xpeer, GROUP1)
            part.copy(device, cpeer, part.core).wait_send()
    for part in mids:
        part.copy(xpeer, cpeer, part.core).wait_send()


def tree_kernel(
    place_ref,
    top_columns,
    mid_columns,
    leaf_columns,
    top_pattern,
    mid_parent,
    leaf_parent,
    mid_pattern,
    leaf_pattern,
    leaf_live,
    root_all,
    tl_all,
    td_all,
    ml_all,
    md_all,
    leaf_lhat,
    leaf_dinv,
    top_diag_out,
    top_coup_out,
    mid_diag_out,
    mid_coup_out,
    leaf_diag_out,
    leaf_coup_out,
    e0h,
    e0l,
    e2h,
    e2l,
    e1h,
    e1l,
    lcat,
    ccat,
    top_c,
    top_d,
):
    me = place_ref[0]
    cols = leaf_dinv.shape[2]
    frame = SLOTS * cols

    per = root_all.shape[1] // cols
    for a in range(per):
        for b in range(per):
            high, low = split(root_all[a * cols : (a + 1) * cols, b * cols : (b + 1) * cols])
            e0h[0, a, b] = high
            e0l[0, a, b] = low

    row_ids = lax.broadcasted_iota(jnp.int32, (cols, cols), 0)
    lane_ids = lax.broadcasted_iota(jnp.int32, (cols, cols), 1)

    def solve(src_h, src_l, source, pattern, lhat, dinv, used, put_coup, put_diag, dst=None):
        keep = lane_ids < used
        for r in range(SLOTS):
            high, low = split(jnp.where(keep, lhat(r), 0.0))
            lcat[r * cols : (r + 1) * cols] = high
            lcat[frame + r * cols : frame + (r + 1) * cols] = low
            lcat[2 * frame + r * cols : 2 * frame + (r + 1) * cols] = high
        for r in range(SLOTS):
            highs = [src_h[source, pattern[r], pattern[k]] for k in range(SLOTS)]
            lows = [src_l[source, pattern[r], pattern[k]] for k in range(SLOTS)]
            wide = jnp.concatenate(highs + highs + lows, axis=1)
            coup = -jnp.dot(wide, lcat[...], preferred_element_type=f32)
            put_coup(r, coup)
            high, low = split(coup)
            ccat[r * cols : (r + 1) * cols] = high
            ccat[frame + r * cols : frame + (r + 1) * cols] = high
            ccat[2 * frame + r * cols : 2 * frame + (r + 1) * cols] = low
            if dst is not None:
                dst_h, dst_l, place_at = dst
                dst_h[place_at, r + 1, 0] = high
                dst_l[place_at, r + 1, 0] = low
                high, low = split(coup.T)
                dst_h[place_at, 0, r + 1] = high
                dst_l[place_at, 0, r + 1] = low
                for k in range(SLOTS):
                    dst_h[place_at, r + 1, k + 1] = highs[k]
                    dst_l[place_at, r + 1, k + 1] = lows[k]
        product = lax.dot_general(
            lcat[...], ccat[...], (((0,), (0,)), ((), ())), preferred_element_type=f32
        )
        diag = jnp.where(keep & (row_ids < used), dinv, 0.0) - product
        put_diag(diag)
        if dst is not None:
            high, low = split(diag)
            dst_h[place_at, 0, 0] = high
            dst_l[place_at, 0, 0] = low

    top_base = me // GROUP2 * NODES2

    def top_step(q, carry):
        pattern = [top_pattern[top_base + q, k] for k in range(SLOTS)]

        def lhat(r):
            return tl_all[pl.ds(pl.multiple_of(q * frame + r * cols, cols), cols)]

        def put_coup(r, value):
            top_c[pl.ds(pl.multiple_of(q * frame + r * cols, cols), cols)] = value

        def put_diag(value):
            top_d[pl.ds(pl.multiple_of(q * cols, cols), cols)] = value

        dinv = td_all[pl.ds(pl.multiple_of(q * cols, cols), cols)]
        used = top_columns[top_base + q]
        solve(e0h, e0l, 0, pattern, lhat, dinv, used, put_coup, put_diag, (e2h, e2l, q))
        return carry

    lax.fori_loop(0, NODES2, top_step, 0)
    member = lax.rem(me, GROUP2)
    rows = top_coup_out.shape[0]
    top_coup_out[...] = top_c[pl.ds(pl.multiple_of(member * rows, 8), rows)]
    rows = top_diag_out.shape[0]
    top_diag_out[...] = top_d[pl.ds(pl.multiple_of(member * rows, 8), rows)]

    leaves = leaf_lhat.shape[0]
    mid_base = me // GROUP1 * GROUP1

    def mid_step(step_index, carry):
        k = leaves - step_index
        leaf = me * leaves + jnp.maximum(k - 1, 0)
        local = jnp.where(k == 0, lax.rem(me, GROUP1), leaf_parent[leaf] - mid_base)
        node = mid_base + local
        pattern = [mid_pattern[node, s] for s in range(SLOTS)]

        def lhat(r):
            return ml_all[pl.ds(pl.multiple_of(local * frame + r * cols, cols), cols)]

        def put_coup(r, value):
            mid_coup_out[r * cols : (r + 1) * cols] = value

        def put_diag(value):
            mid_diag_out[...] = value

        dinv = md_all[pl.ds(pl.multiple_of(local * cols, cols), cols)]
        source = mid_parent[node] - top_base
        solve(
            e2h, e2l, source, pattern, lhat, dinv, mid_columns[node], put_coup, put_diag,
            (e1h, e1l, k),
        )
        return carry

    lax.fori_loop(0, leaves + 1, mid_step, 0)

    def leaf_step(i, carry):
        node = me * leaves + i
        pattern = [leaf_pattern[node, s] for s in range(SLOTS)]
        live = jnp.full((cols, cols), i, jnp.int32) < leaf_live[me]

        def lhat(r):
            return leaf_lhat[i, r * cols : (r + 1) * cols]

        def put_coup(r, value):
            leaf_coup_out[i, r * cols : (r + 1) * cols] = jnp.where(live, value, 0.0)

        def put_diag(value):
            leaf_diag_out[i] = jnp.where(live, value, 0.0)

        solve(e1h, e1l, i + 1, pattern, lhat, leaf_dinv[i], leaf_columns[node], put_coup, put_diag)
        return carry

    lax.fori_loop(0, leaves, leaf_step, 0)


def body(
    root_frame,
    top_lhat,
    top_dinv,
    mid_lhat,
    mid_dinv,
    leaf_lhat,
    leaf_dinv,
    *scalars,
):
    n = lax.axis_size("leaf")
    cols = top_dinv.shape[1]
    frame = SLOTS * cols
    per = root_frame.shape[1] // cols
    leaves = leaf_lhat.shape[0]
    grid = SLOTS + 1

    def dma(count):
        return pltpu.SemaphoreType.DMA((count,))

    sems = []
    for group in (n, GROUP2, GROUP2, GROUP1, GROUP1):
        sems += [dma(group) for _ in range(5)] + [dma(1)]
    vmem = pl.BlockSpec(memory_space=pltpu.VMEM)
    smem = pl.BlockSpec(memory_space=pltpu.SMEM)
    anywhere = pl.BlockSpec(memory_space=pl.ANY)
    mine = (root_frame, top_lhat, top_dinv, mid_lhat[0], mid_dinv[0])
    groups = (n, GROUP2, GROUP2, GROUP1, GROUP1)
    whole = pl.pallas_call(
        functools.partial(gather_kernel, n),
        out_shape=[
            jax.ShapeDtypeStruct((count * x.shape[0], x.shape[1]), f32)
            for count, x in zip(groups, mine)
        ],
        in_specs=[anywhere] * 5,
        out_specs=[anywhere] * 5,
        scratch_shapes=sems,
        compiler_params=pltpu.CompilerParams(
            collective_id=0, has_side_effects=True, vmem_limit_bytes=1024 * 1024
        ),
    )(*mine)
    outs = pl.pallas_call(
        tree_kernel,
        out_shape=[
            jax.ShapeDtypeStruct(top_dinv.shape, f32),
            jax.ShapeDtypeStruct(top_lhat.shape, f32),
            jax.ShapeDtypeStruct(mid_dinv.shape[1:], f32),
            jax.ShapeDtypeStruct(mid_lhat.shape[1:], f32),
            jax.ShapeDtypeStruct(leaf_dinv.shape, f32),
            jax.ShapeDtypeStruct(leaf_lhat.shape, f32),
        ],
        in_specs=[smem] * 10 + [vmem] * 7,
        out_specs=[vmem] * 6,
        scratch_shapes=[
            pltpu.VMEM((1, per, per, cols, cols), bf16),
            pltpu.VMEM((1, per, per, cols, cols), bf16),
            pltpu.VMEM((NODES2, grid, grid, cols, cols), bf16),
            pltpu.VMEM((NODES2, grid, grid, cols, cols), bf16),
            pltpu.VMEM((leaves + 1, grid, grid, cols, cols), bf16),
            pltpu.VMEM((leaves + 1, grid, grid, cols, cols), bf16),
            pltpu.VMEM((3 * frame, cols), bf16),
            pltpu.VMEM((3 * frame, cols), bf16),
            pltpu.VMEM((NODES2 * frame, cols), f32),
            pltpu.VMEM((NODES2 * cols, cols), f32),
        ],
        compiler_params=pltpu.CompilerParams(vmem_limit_bytes=36 * 1024 * 1024),
    )(lax.axis_index("leaf").reshape(1).astype(jnp.int32), *scalars, *whole, leaf_lhat, leaf_dinv)
    return (outs[0], outs[1], outs[2][None], outs[3][None], outs[4], outs[5])


def solution(mesh):
    rows = P(("pole", "leaf"), None)
    stacks = P(("pole", "leaf"), None, None)
    in_specs = (rows,) * 3 + (stacks,) * 4 + (P(),) * 9
    out_specs = (rows,) * 2 + (stacks,) * 4
    return jax.shard_map(body, mesh=mesh, in_specs=in_specs, out_specs=out_specs, check_vma=False)
```

```python
import functools

import jax
import jax.numpy as jnp
from jax import lax
from jax.experimental import pallas as pl
from jax.experimental.pallas import tpu as pltpu
from jax.sharding import PartitionSpec as P

SLOTS = 3
GROUP2 = 16
NODES2 = 2
GROUP1 = 4

MESH = pl.DeviceIdType.MESH
f32 = jnp.float32
bf16 = jnp.bfloat16


def split(value):
    high = value.astype(bf16)
    low = (value - high.astype(f32)).astype(bf16)
    return high, low


def remote(src, dst, send_sem, recv_sem, target):
    return pltpu.make_async_remote_copy(
        src_ref=src,
        dst_ref=dst,
        send_sem=send_sem,
        recv_sem=recv_sem,
        device_id={"leaf": target},
        device_id_type=MESH,
    )


def in_hbm(x):
    return pltpu.with_memory_space_constraint(x, pltpu.HBM)


class Spread:
    def __init__(self, own, whole, group, sems, me, valid=None):
        self.own, self.whole, self.group = own, whole, group
        self.valid = valid
        self.rows = own.shape[0]
        self.recv, self.up, self.down, self.side, self.core, self.local = sems
        self.base = me - lax.rem(me, group)

    def block(self, device):
        start = (device - self.base) * self.rows
        return self.whole.at[pl.ds(pl.multiple_of(start, 8), self.rows)]

    def copy(self, device, target, sems, own=False):
        slot = device - self.base
        return remote(
            self.own if own else self.block(device),
            self.block(device),
            sems.at[slot],
            self.recv.at[slot],
            target,
        )

    def keep(self, me):
        return pltpu.make_async_copy(self.own, self.block(me), self.local.at[0])

    def arrived(self, device, me):
        self.copy(device, me, self.core).wait_recv()


def gather_kernel(
    n,
    pieces,
    root_in,
    tl_in,
    td_in,
    ml_in,
    md_in,
    *rest,
):
    root_alls, rest = rest[:pieces], rest[pieces:]
    tl_all, td_all, ml_all, md_all = rest[:4]
    sems = rest[4:]
    me = lax.axis_index("leaf")
    core = lax.rem(me, 2)
    side = lax.rem(me // 2, 2)
    cpeer = me + 1 - 2 * core
    xpeer = me + 2 - 4 * side
    cols = td_in.shape[1]
    root_rows = root_in.shape[0]
    per = root_in.shape[1] // cols
    block_row = me * root_rows // cols

    def in_half(device):
        return device * root_rows // cols < per // 2

    roots = []
    for k in range(pieces):
        column = pl.multiple_of(lax.rem(block_row + k, per) * cols, cols)
        roots.append(
            Spread(
                root_in.at[:, pl.ds(column, cols)],
                root_alls[k],
                n,
                sems[6 * k : 6 * k + 6],
                me,
                in_half if k == per // 2 else None,
            )
        )
    sems = sems[6 * pieces :]
    tl = Spread(tl_in, tl_all, GROUP2, sems[0:6], me)
    td = Spread(td_in, td_all, GROUP2, sems[6:12], me)
    ml = Spread(ml_in, ml_all, GROUP1, sems[12:18], me)
    md = Spread(md_in, md_all, GROUP1, sems[18:24], me)
    tops = (tl, td)
    mids = (ml, md)

    line = n // GROUP1
    place = me // GROUP1
    top_line = GROUP2 // GROUP1
    top_place = lax.rem(me, GROUP2) // GROUP1
    has_up = place < line - 1
    has_down = place > 0

    barrier = pltpu.get_barrier_semaphore()
    for peer in (cpeer, xpeer):
        pl.semaphore_signal(barrier, inc=1, device_id={"leaf": peer}, device_id_type=MESH)

    @pl.when(has_up)
    def _():
        pl.semaphore_signal(barrier, inc=1, device_id={"leaf": me + GROUP1}, device_id_type=MESH)

    @pl.when(has_down)
    def _():
        pl.semaphore_signal(barrier, inc=1, device_id={"leaf": me - GROUP1}, device_id_type=MESH)

    def when(part, device, act):
        if part.valid is None:
            act()
        else:
            pl.when(part.valid(device))(act)

    for part in tops + mids:
        part.keep(me).start()
    for part in roots:
        when(part, me, lambda: part.keep(me).start())
    peers = 2 + jnp.minimum(place, 1) + jnp.minimum(line - 1 - place, 1)
    pl.semaphore_wait(barrier, peers)

    def along(part, device, go_up, ok, act, own=False):
        if go_up:
            @pl.when(ok)
            def _():
                act(part.copy(device, me + GROUP1, part.up, own))
        else:
            @pl.when(ok)
            def _():
                act(part.copy(device, me - GROUP1, part.down, own))

    def start(copy):
        copy.start()

    def wait_send(copy):
        copy.wait_send()

    top_up = top_place < top_line - 1
    top_down = top_place > 0

    def root_line(device, go_up, act, own=False):
        for part in roots:
            def go():
                along(part, device, go_up, has_up if go_up else has_down, act, own)

            when(part, device, go)

    def root_to(device, target, core_way, act, own=False):
        for part in roots:
            def go():
                act(part.copy(device, target, part.core if core_way else part.side, own))

            when(part, device, go)

    def root_arrived(device):
        for part in roots:
            when(part, device, lambda: part.arrived(device, me))

    def own_copies(act):
        root_to(me, xpeer, False, act, True)
        for part in tops:
            along(part, me, True, top_up, act, True)
            along(part, me, False, top_down, act, True)
        root_line(me, True, act, True)
        root_line(me, False, act, True)
        for part in tops:
            act(part.copy(me, xpeer, part.side, True))
        root_to(me, cpeer, True, act, True)
        for part in tops:
            act(part.copy(me, cpeer, part.core, True))
        for part in mids:
            act(part.copy(me, xpeer, part.side, True))
            act(part.copy(me, cpeer, part.core, True))

    own_copies(start)

    root_arrived(xpeer)
    root_line(xpeer, True, start)
    root_line(xpeer, False, start)
    root_to(xpeer, cpeer, True, start)

    def step(s, carry):
        for go_up in (True, False):
            shift = -s * GROUP1 if go_up else s * GROUP1
            got_top = (top_place >= s) if go_up else (top_place + s < top_line)
            got_root = (place >= s) if go_up else (place + s < line)

            @pl.when(got_top)
            def _():
                for part in tops:
                    part.arrived(me + shift, me)
                    along(part, me + shift, go_up, top_up if go_up else top_down, start)
                    part.copy(me + shift, xpeer, part.side).start()
                    part.copy(me + shift, cpeer, part.core).start()

            @pl.when(got_root)
            def _():
                for device in (me, xpeer):
                    root_arrived(device + shift)
                    root_line(device + shift, go_up, start)
                    root_to(device + shift, cpeer, True, start)

        return carry

    lax.fori_loop(1, line, step, 0)

    for part in tops:
        for q in range(top_line):
            device = part.base + q * GROUP1 + lax.rem(xpeer, GROUP1)
            part.arrived(device, me)
            part.copy(device, cpeer, part.core).start()
    for part in tuple(roots) + tops:
        def other(q, carry):
            for peer in (cpeer, cpeer + xpeer - me):
                device = part.base + q * GROUP1 + lax.rem(peer, GROUP1)
                when(part, device, lambda: part.arrived(device, me))
            return carry

        lax.fori_loop(0, part.group // GROUP1, other, 0)
        when(part, me, lambda: part.keep(me).wait())

    for part in mids:
        part.arrived(xpeer, me)
        part.copy(xpeer, cpeer, part.core).start()
    for part in mids:
        part.arrived(cpeer, me)
        part.arrived(cpeer + xpeer - me, me)
        part.keep(me).wait()

    own_copies(wait_send)
    root_line(xpeer, True, wait_send)
    root_line(xpeer, False, wait_send)
    root_to(xpeer, cpeer, True, wait_send)

    def drain(s, carry):
        for go_up in (True, False):
            shift = -s * GROUP1 if go_up else s * GROUP1
            got_top = (top_place >= s) if go_up else (top_place + s < top_line)
            got_root = (place >= s) if go_up else (place + s < line)

            @pl.when(got_top)
            def _():
                for part in tops:
                    along(part, me + shift, go_up, top_up if go_up else top_down, wait_send)
                    part.copy(me + shift, xpeer, part.side).wait_send()
                    part.copy(me + shift, cpeer, part.core).wait_send()

            @pl.when(got_root)
            def _():
                for device in (me, xpeer):
                    root_line(device + shift, go_up, wait_send)
                    root_to(device + shift, cpeer, True, wait_send)

        return carry

    lax.fori_loop(1, line, drain, 0)
    for part in tops:
        for q in range(top_line):
            device = part.base + q * GROUP1 + lax.rem(xpeer, GROUP1)
            part.copy(device, cpeer, part.core).wait_send()
    for part in mids:
        part.copy(xpeer, cpeer, part.core).wait_send()


def tree_kernel(pieces, *refs):
    small_in, mid_pattern, leaf_pattern = refs[:7], refs[7], refs[8]
    root_alls, refs = refs[9 : 9 + pieces], refs[9 + pieces :]
    tl_all, td_all, ml_all, md_all, leaf_lhat_in, leaf_dinv_in = refs[:6]
    (
        top_diag_out,
        top_coup_out,
        mid_diag_out,
        mid_coup_out,
        leaf_diag_out,
        leaf_coup_out,
    ) = refs[6:12]
    e0h, e0l, e2h, e2l, e1h, e1l, lcat, ccat, top_c, top_d, leaf_lhat, leaf_dinv = refs[12:24]
    small = refs[24:31]
    sems = refs[31]
    top_columns, mid_columns, leaf_columns, top_pattern, mid_parent, leaf_parent, leaf_live = small
    fetched = list(zip(small_in + (leaf_lhat_in, leaf_dinv_in), small + (leaf_lhat, leaf_dinv)))
    fetches = [pltpu.make_async_copy(a, b, sems.at[i]) for i, (a, b) in enumerate(fetched)]
    for fetch in fetches:
        fetch.start()
    me = lax.axis_index("leaf")
    cols = leaf_dinv.shape[2]
    frame = SLOTS * cols

    per = e0h.shape[1]
    for k in range(pieces):
        for a in range(per // 2 if k == per // 2 else per):
            b = (a + k) % per
            value = root_alls[k][a * cols : (a + 1) * cols]
            e0h[0, a, b], e0l[0, a, b] = split(value)
            if k:
                e0h[0, b, a], e0l[0, b, a] = split(value.T)
    for fetch in fetches[:-2]:
        fetch.wait()

    row_ids = lax.broadcasted_iota(jnp.int32, (cols, cols), 0)
    lane_ids = lax.broadcasted_iota(jnp.int32, (cols, cols), 1)

    def solve(src_h, src_l, source, pattern, lhat, dinv, used, put_coup, put_diag, dst=None):
        keep = lane_ids < used
        for r in range(SLOTS):
            high, low = split(jnp.where(keep, lhat(r), 0.0))
            lcat[r * cols : (r + 1) * cols] = high
            lcat[frame + r * cols : frame + (r + 1) * cols] = low
            lcat[2 * frame + r * cols : 2 * frame + (r + 1) * cols] = high
        for r in range(SLOTS):
            highs = [src_h[source, pattern[r], pattern[k]] for k in range(SLOTS)]
            lows = [src_l[source, pattern[r], pattern[k]] for k in range(SLOTS)]
            wide = jnp.concatenate(highs + highs + lows, axis=1)
            coup = -jnp.dot(wide, lcat[...], preferred_element_type=f32)
            put_coup(r, coup)
            high, low = split(coup)
            ccat[r * cols : (r + 1) * cols] = high
            ccat[frame + r * cols : frame + (r + 1) * cols] = high
            ccat[2 * frame + r * cols : 2 * frame + (r + 1) * cols] = low
            if dst is not None:
                dst_h, dst_l, place_at = dst
                dst_h[place_at, r + 1, 0] = high
                dst_l[place_at, r + 1, 0] = low
                high, low = split(coup.T)
                dst_h[place_at, 0, r + 1] = high
                dst_l[place_at, 0, r + 1] = low
                for k in range(SLOTS):
                    dst_h[place_at, r + 1, k + 1] = highs[k]
                    dst_l[place_at, r + 1, k + 1] = lows[k]
        product = lax.dot_general(
            lcat[...], ccat[...], (((0,), (0,)), ((), ())), preferred_element_type=f32
        )
        diag = jnp.where(keep & (row_ids < used), dinv, 0.0) - product
        put_diag(diag)
        if dst is not None:
            high, low = split(diag)
            dst_h[place_at, 0, 0] = high
            dst_l[place_at, 0, 0] = low

    top_base = me // GROUP2 * NODES2

    def top_step(q, carry):
        pattern = [top_pattern[top_base + q, k] for k in range(SLOTS)]

        def lhat(r):
            return tl_all[pl.ds(pl.multiple_of(q * frame + r * cols, cols), cols)]

        def put_coup(r, value):
            top_c[pl.ds(pl.multiple_of(q * frame + r * cols, cols), cols)] = value

        def put_diag(value):
            top_d[pl.ds(pl.multiple_of(q * cols, cols), cols)] = value

        dinv = td_all[pl.ds(pl.multiple_of(q * cols, cols), cols)]
        used = top_columns[top_base + q]
        solve(e0h, e0l, 0, pattern, lhat, dinv, used, put_coup, put_diag, (e2h, e2l, q))
        return carry

    lax.fori_loop(0, NODES2, top_step, 0)
    member = lax.rem(me, GROUP2)
    rows = top_coup_out.shape[0]
    top_coup_out[...] = top_c[pl.ds(pl.multiple_of(member * rows, 8), rows)]
    rows = top_diag_out.shape[0]
    top_diag_out[...] = top_d[pl.ds(pl.multiple_of(member * rows, 8), rows)]

    leaves = leaf_lhat.shape[0]
    mid_base = me // GROUP1 * GROUP1

    def mid_step(step_index, carry):
        k = leaves - step_index
        leaf = me * leaves + jnp.maximum(k - 1, 0)
        local = jnp.where(k == 0, lax.rem(me, GROUP1), leaf_parent[leaf] - mid_base)
        node = mid_base + local
        pattern = [mid_pattern[node, s] for s in range(SLOTS)]

        def lhat(r):
            return ml_all[pl.ds(pl.multiple_of(local * frame + r * cols, cols), cols)]

        def put_coup(r, value):
            mid_coup_out[r * cols : (r + 1) * cols] = value

        def put_diag(value):
            mid_diag_out[...] = value

        dinv = md_all[pl.ds(pl.multiple_of(local * cols, cols), cols)]
        source = mid_parent[node] - top_base
        solve(
            e2h, e2l, source, pattern, lhat, dinv, mid_columns[node], put_coup, put_diag,
            (e1h, e1l, k),
        )
        return carry

    lax.fori_loop(0, leaves + 1, mid_step, 0)

    for fetch in fetches[-2:]:
        fetch.wait()

    def leaf_step(i, carry):
        node = me * leaves + i
        pattern = [leaf_pattern[node, s] for s in range(SLOTS)]
        live = jnp.full((cols, cols), i, jnp.int32) < leaf_live[me]

        def lhat(r):
            return leaf_lhat[i, r * cols : (r + 1) * cols]

        def put_coup(r, value):
            leaf_coup_out[i, r * cols : (r + 1) * cols] = jnp.where(live, value, 0.0)

        def put_diag(value):
            leaf_diag_out[i] = jnp.where(live, value, 0.0)

        solve(e1h, e1l, i + 1, pattern, lhat, leaf_dinv[i], leaf_columns[node], put_coup, put_diag)
        return carry

    lax.fori_loop(0, leaves, leaf_step, 0)


def body(
    root_frame,
    top_lhat,
    top_dinv,
    mid_lhat,
    mid_dinv,
    leaf_lhat,
    leaf_dinv,
    *scalars,
):
    n = lax.axis_size("leaf")
    cols = top_dinv.shape[1]
    frame = SLOTS * cols
    per = root_frame.shape[1] // cols
    leaves = leaf_lhat.shape[0]
    grid = SLOTS + 1

    def dma(count):
        return pltpu.SemaphoreType.DMA((count,))

    pieces = per // 2 + 1
    sems = []
    for group in (n,) * pieces + (GROUP2, GROUP2, GROUP1, GROUP1):
        sems += [dma(group) for _ in range(5)] + [dma(1)]
    vmem = pl.BlockSpec(memory_space=pltpu.VMEM)
    smem = pl.BlockSpec(memory_space=pltpu.SMEM)
    anywhere = pl.BlockSpec(memory_space=pl.ANY)
    mine = (root_frame, top_lhat, top_dinv, mid_lhat[0], mid_dinv[0])
    groups = (GROUP2, GROUP2, GROUP1, GROUP1)
    root_rows = n * root_frame.shape[0]
    root_shapes = [
        jax.ShapeDtypeStruct((root_rows // 2 if k == per // 2 else root_rows, cols), f32)
        for k in range(pieces)
    ]
    hbm = pl.BlockSpec(memory_space=pltpu.HBM)
    whole = pl.pallas_call(
        functools.partial(gather_kernel, n, pieces),
        out_shape=root_shapes
        + [
            jax.ShapeDtypeStruct((count * x.shape[0], x.shape[1]), f32)
            for count, x in zip(groups, mine[1:])
        ],
        in_specs=[hbm] * 5,
        out_specs=[anywhere] * (pieces + 4),
        scratch_shapes=sems,
        compiler_params=pltpu.CompilerParams(
            collective_id=0, has_side_effects=True, vmem_limit_bytes=1024 * 1024
        ),
    )(*[in_hbm(x) for x in mine])
    small = scalars[:6] + scalars[8:]
    outs = pl.pallas_call(
        functools.partial(tree_kernel, pieces),
        out_shape=[
            jax.ShapeDtypeStruct(top_dinv.shape, f32),
            jax.ShapeDtypeStruct(top_lhat.shape, f32),
            jax.ShapeDtypeStruct(mid_dinv.shape[1:], f32),
            jax.ShapeDtypeStruct(mid_lhat.shape[1:], f32),
            jax.ShapeDtypeStruct(leaf_dinv.shape, f32),
            jax.ShapeDtypeStruct(leaf_lhat.shape, f32),
        ],
        in_specs=[hbm] * 7 + [smem] * 2 + [vmem] * (pieces + 4) + [hbm] * 2,
        out_specs=[vmem] * 6,
        scratch_shapes=[
            pltpu.VMEM((1, per, per, cols, cols), bf16),
            pltpu.VMEM((1, per, per, cols, cols), bf16),
            pltpu.VMEM((NODES2, grid, grid, cols, cols), bf16),
            pltpu.VMEM((NODES2, grid, grid, cols, cols), bf16),
            pltpu.VMEM((leaves + 1, grid, grid, cols, cols), bf16),
            pltpu.VMEM((leaves + 1, grid, grid, cols, cols), bf16),
            pltpu.VMEM((3 * frame, cols), bf16),
            pltpu.VMEM((3 * frame, cols), bf16),
            pltpu.VMEM((NODES2 * frame, cols), f32),
            pltpu.VMEM((NODES2 * cols, cols), f32),
            pltpu.VMEM(leaf_lhat.shape, f32),
            pltpu.VMEM(leaf_dinv.shape, f32),
        ]
        + [pltpu.SMEM(x.shape, jnp.int32) for x in small]
        + [dma(len(small) + 2)],
        compiler_params=pltpu.CompilerParams(vmem_limit_bytes=36 * 1024 * 1024),
    )(
        *[in_hbm(x) for x in small], scalars[6], scalars[7], *whole, in_hbm(leaf_lhat), in_hbm(leaf_dinv)
    )
    return (outs[0], outs[1], outs[2][None], outs[3][None], outs[4], outs[5])


def solution(mesh):
    rows = P(("pole", "leaf"), None)
    stacks = P(("pole", "leaf"), None, None)
    in_specs = (rows,) * 3 + (stacks,) * 4 + (P(),) * 9
    out_specs = (rows,) * 2 + (stacks,) * 4
    return jax.shard_map(body, mesh=mesh, in_specs=in_specs, out_specs=out_specs, check_vma=False)
```
